32 devices in a mesh: gx: 4 (over y, x), gy: 8 (over z, core).
Axes of the slice: x: 2, y: 2, z: 4, core: 2. Of those that a mesh axis runs over, the one named last changes fastest.
Arguments:
- position: float32 [2, 24, 48, 128], P(None, 'gx', 'gy'), may hold values from 0 to 1
- velocity: float32 [2, 24, 48, 128], P(None, 'gx', 'gy'), may hold values from -3 to 3
- other_accel: float32 [2, 24, 48, 128], P(None, 'gx', 'gy'), may hold values from -5 to 5
- phase_ids: int32 [24, 48, 128], P('gx', 'gy'), may hold values from 0 to 1, as said below
- counts: int32 [24, 48], P('gx', 'gy'), may hold values from 48 to 128, as said below
Outputs:
- new_position: float32 [2, 24, 48, 128], P(None, 'gx', 'gy')
- new_velocity: float32 [2, 24, 48, 128], P(None, 'gx', 'gy')
- pressure: float32 [24, 48, 128], P('gx', 'gy')
- monitor: float32 [4, 4], replicated
The draws below stay inside these ranges and needn't reach their ends.
Inputs may be any that keep to these rules, and one draw needn't show every extreme that they name: `counts`: each entry is the number of live slots of its cell; the live slots are the first ones of the cell; some cell holds 128. `phase_ids`: both phases occur among the live slots.
All inputs are finite; a program needn't handle non-finite values.
Results may differ from the reference program's by a relative error of at most 0.0001.
Values sent between devices are 32-bit elements; how exact they have to be, the bound alone decides.
A program may use at most 64 MiB of HBM per device.

```python
import jax
import jax.numpy as jnp
from jax import lax

SLOTS = 128
ITERS = 4
CELLS_X = 24
CELLS_Y = 48


def draw_counts(key, part):
    values = jax.random.randint(key, (CELLS_X, CELLS_Y), 48, SLOTS + 1, dtype=jnp.int32)
    return values.at[0, 0].set(SLOTS)


def draw_phase_ids(key, part):
    values = jax.random.randint(key, (CELLS_X, CELLS_Y, SLOTS), 0, 2, dtype=jnp.int32)
    return values.at[0, 0, 0].set(0).at[0, 0, 1].set(1)


def block_scale(own_key, dims, pieces, smallest, largest):
    factor_of = 1.0
    for axis_at, parts in pieces:
        draws = jax.random.uniform(jax.random.fold_in(jax.random.fold_in(own_key, 6), axis_at), (parts,), jnp.float32, smallest / len(pieces), largest / len(pieces))
        factor_of = factor_of * jnp.repeat(jnp.exp(draws), dims[axis_at] // parts).reshape((-1,) + (1,) * (len(dims) - 1 - axis_at))
    return factor_of


def gaussian(own_key, dims, deviation, reach, split=(), kind=jnp.bfloat16):
    drawn = jax.random.normal(own_key, dims, jnp.float32) * deviation
    if len(split) > 0:
        drawn = block_scale(own_key, dims, split, -0.22, 0.18) * drawn
    return jnp.clip(drawn, min=-reach, max=reach).astype(kind)


def setup_inputs(seed: int = 0) -> dict:
    seeds = jax.random.split(jax.random.key(seed), 6)
    position = jnp.clip(1.0 * jax.random.uniform(seeds[0], (2, CELLS_X, CELLS_Y, SLOTS), jnp.float32) ** block_scale(seeds[0], (2, CELLS_X, CELLS_Y, SLOTS), ((1, 4), (2, 8)), -0.2, 0.2), 0.0, 1.0)
    velocity = gaussian(seeds[1], (2, CELLS_X, CELLS_Y, SLOTS), 0.5, 3.0, ((1, 4), (2, 8)), jnp.float32)
    other_accel = gaussian(seeds[2], (2, CELLS_X, CELLS_Y, SLOTS), 1.0, 5.0, ((1, 4), (2, 8)), jnp.float32)
    phase_ids = draw_phase_ids(jax.random.fold_in(seeds[5], 71), 0)
    counts = draw_counts(jax.random.fold_in(seeds[5], 71), 0)
    return {"position": position, "velocity": velocity, "other_accel": other_accel, "phase_ids": phase_ids, "counts": counts}


TIME_STEP = 0.05
KERNEL_NORM = 4.0 / (3.141592653589793 * 64.0)
REST_LIGHT = 1.2
REST_HEAVY = 1.5
STIFF_LIGHT = 100.0
STIFF_HEAVY = 200.0
MASS_LIGHT = 1.0
MASS_HEAVY = 1.5
SENTINEL = 1.0e30


def window_of(source, off_x, off_y, row_count, col_count):
    return source[1 + off_x:1 + off_x + row_count, 1 + off_y:1 + off_y + col_count]


def pair_sums(centers, padded_list, with_force):
    center_x, center_y = centers[0], centers[1]
    near_x, near_y, near_live = padded_list[0], padded_list[1], padded_list[2]
    row_count, col_count = center_x.shape[0], center_x.shape[1]
    total_a = jnp.zeros_like(center_x)
    total_b = jnp.zeros_like(center_x)
    for off_x in (-1, 0, 1):
        for off_y in (-1, 0, 1):
            other_x = window_of(near_x, off_x, off_y, row_count, col_count)
            other_y = window_of(near_y, off_x, off_y, row_count, col_count)
            other_live = window_of(near_live, off_x, off_y, row_count, col_count)
            diff_x = center_x[..., :, None] - (other_x[..., None, :] + off_x)
            diff_y = center_y[..., :, None] - (other_y[..., None, :] + off_y)
            intersection = jnp.maximum(1.0 - diff_x * diff_x - diff_y * diff_y, 0.0) * other_live[..., None, :]
            if with_force:
                other_term = window_of(padded_list[3], off_x, off_y, row_count, col_count)
                pair_coef = intersection * intersection * (centers[2][..., :, None] + other_term[..., None, :])
                total_a = total_a + jnp.sum(pair_coef * diff_x, axis=-1)
                total_b = total_b + jnp.sum(pair_coef * diff_y, axis=-1)
            else:
                total_a = total_a + jnp.sum(intersection * intersection * intersection, axis=-1)
    if with_force:
        return (total_a, total_b)
    return (total_a,)


def blocked(with_force, centers, padded_list, row_count):
    block_count = row_count // 2

    def one_block(block_index):
        first_row = block_index * 2
        center_part = tuple(lax.dynamic_slice_in_dim(source, first_row, 2, 0) for source in centers)
        padded_part = tuple(lax.dynamic_slice_in_dim(source, first_row, 4, 0) for source in padded_list)
        return pair_sums(center_part, padded_part, with_force)

    results = lax.map(one_block, jnp.arange(block_count, dtype=jnp.int32))
    return tuple(source.reshape((row_count,) + source.shape[2:]) for source in results)


def local_bounds(density_ratio, live_bool, heavy_bool):
    light_sel = live_bool & jnp.logical_not(heavy_bool)
    heavy_sel = live_bool & heavy_bool
    top_ratio = jnp.stack([jnp.max(jnp.where(light_sel, density_ratio, -SENTINEL)),
                           jnp.max(jnp.where(heavy_sel, density_ratio, -SENTINEL))])
    low_ratio = jnp.stack([jnp.min(jnp.where(light_sel, density_ratio, SENTINEL)),
                           jnp.min(jnp.where(heavy_sel, density_ratio, SENTINEL))])
    return top_ratio, low_ratio


def wrapped(source):
    return jnp.pad(source, ((1, 1), (1, 1), (0, 0)), mode="wrap")


def reference(position, velocity, other_accel, phase_ids, counts):
    slot_index = jnp.arange(position.shape[-1], dtype=jnp.int32)
    live_bool = slot_index[None, None, :] < counts[:, :, None]
    heavy_bool = phase_ids == 1
    live_mask = live_bool.astype(jnp.float32)
    rest_density = jnp.where(heavy_bool, REST_HEAVY, REST_LIGHT).astype(jnp.float32)
    stiffness = jnp.where(heavy_bool, STIFF_HEAVY, STIFF_LIGHT).astype(jnp.float32)
    particle_mass = jnp.where(heavy_bool, MASS_HEAVY, MASS_LIGHT).astype(jnp.float32)
    pressure = jnp.zeros_like(live_mask)
    accel_x = jnp.zeros_like(live_mask)
    accel_y = jnp.zeros_like(live_mask)
    monitor_rows = []
    row_total = position.shape[1]
    for iteration in range(ITERS):
        vel_x = velocity[0] + TIME_STEP * (other_accel[0] + accel_x)
        vel_y = velocity[1] + TIME_STEP * (other_accel[1] + accel_y)
        pos_x = position[0] + TIME_STEP * vel_x
        pos_y = position[1] + TIME_STEP * vel_y
        (density_sum,) = blocked(False, (pos_x, pos_y), (wrapped(pos_x), wrapped(pos_y), wrapped(live_mask)), row_total)
        density = KERNEL_NORM * density_sum
        density_ratio = density / rest_density
        top_ratio, low_ratio = local_bounds(density_ratio, live_bool, heavy_bool)
        relaxation = 1.0 / (1.0 + top_ratio - low_ratio)
        particle_relax = jnp.where(heavy_bool, relaxation[1], relaxation[0])
        pressure = live_mask * (pressure + stiffness * particle_relax * (density_ratio - 1.0))
        safe_density = jnp.where(live_bool, density, 1.0)
        press_term = jnp.where(live_bool, pressure / (safe_density * safe_density), 0.0)
        force_x, force_y = blocked(True, (pos_x, pos_y, press_term),
                                   (wrapped(pos_x), wrapped(pos_y), wrapped(live_mask), wrapped(press_term)), row_total)
        accel_x = live_mask * (6.0 * KERNEL_NORM / particle_mass) * force_x
        accel_y = live_mask * (6.0 * KERNEL_NORM / particle_mass) * force_y
        monitor_rows.append(jnp.concatenate([top_ratio, low_ratio]))
    new_vel_x = live_mask * (velocity[0] + TIME_STEP * (other_accel[0] + accel_x))
    new_vel_y = live_mask * (velocity[1] + TIME_STEP * (other_accel[1] + accel_y))
    new_pos_x = live_mask * (position[0] + TIME_STEP * new_vel_x)
    new_pos_y = live_mask * (position[1] + TIME_STEP * new_vel_y)
    return (jnp.stack([new_pos_x, new_pos_y]), jnp.stack([new_vel_x, new_vel_y]), pressure, jnp.stack(monitor_rows))
```

```python
import functools

import jax
import jax.numpy as jnp
from jax import lax
from jax.experimental import pallas as pl
from jax.experimental.pallas import tpu as pltpu
from jax.sharding import PartitionSpec as P

ITERS = 4


TIME_STEP = 0.05
KERNEL_NORM = 4.0 / (3.141592653589793 * 64.0)
REST_LIGHT = 1.2
REST_HEAVY = 1.5
STIFF_LIGHT = 100.0
STIFF_HEAVY = 200.0
MASS_LIGHT = 1.0
MASS_HEAVY = 1.5
SENTINEL = 1e30


EMPTY = -1e30
FAR = 1e30
LIMIT = 1e29
DIAGONALS = tuple((dx, dy) for dx in (-1, 1) for dy in (-1, 1))
SIDES = ((-1, 0), (1, 0), (0, -1), (0, 1))
DIRS = DIAGONALS + SIDES


def rounded(value):
    return value.astype(jnp.bfloat16).astype(jnp.float32)


def split2(value):
    high = rounded(value)
    return high, rounded(value - high)


def split3(value):
    high = rounded(value)
    rest = value - high
    mid = rounded(rest)
    return high, mid, rounded(rest - mid)


def put_rows(ref, at, values, width):
    for k, value in enumerate(values):
        ref[at, k * width : (k + 1) * width, :] = value


def source_features(x, y, ref, at, width):
    live = x < LIMIT
    x = jnp.where(live, x - 0.5, 0.0)
    y = jnp.where(live, y - 0.5, 0.0)
    xh, xm, xl = split3(x)
    yh, ym, yl = split3(y)
    bh, bm, bl = split3(jnp.where(live, -(x * x + y * y), EMPTY))
    put_rows(
        ref,
        at,
        [xh, xh, xm, xh, xl, xm, bh, bm, yh, yh, ym, yh, yl, ym, bl],
        width,
    )


def source_constants(ref, at, width, like):
    nil, one = jnp.zeros_like(like), jnp.ones_like(like)
    for k in range(15, 24):
        ref[at, k * width : (k + 1) * width, :] = one if 16 <= k <= 18 else nil


def target_features(x, y, xf, yf, af, row, width):
    x = jnp.where(x < LIMIT, x, 0.0) - 0.5
    y = y - 0.5
    for at in range(3):
        h, m, l = split3(2.0 * (x - (at - 1.0)))
        put_rows(xf.at[row], at, [h, m, h, l, h, m], width)
        h, m, l = split3(2.0 * (y - (at - 1.0)))
        put_rows(yf.at[row], at, [h, m, h, l, h, m], width)
    for ax in range(3):
        for ay in range(3):
            dx = x - (ax - 1.0)
            dy = y - (ay - 1.0)
            put_rows(af.at[row], 3 * ax + ay, split3(1.0 - (dx * dx + dy * dy)), width)


def target_constants(xf, yf, af, row, width, like):
    nil, one = jnp.zeros_like(like), jnp.ones_like(like)
    for at in range(3):
        for ref, values in ((xf, (one, one)), (yf, (one, nil))):
            for k, value in enumerate(values):
                ref[row, at, (6 + k) * width : (7 + k) * width, :] = value
    for at in range(9):
        for k in range(3, 8):
            af[row, at, k * width : (k + 1) * width, :] = nil


def value_rows(x, y, parts, ref, at, width):
    live = x < LIMIT
    x = jnp.where(live, x - 0.5, 0.0)
    y = jnp.where(live, y - 0.5, 0.0)
    parts = [jnp.where(live, part, 0.0) for part in parts]
    splits = [split2(part) for part in parts]
    one = jnp.where(live, 1.0, 0.0)
    nil = jnp.zeros_like(x)
    groups = [[one] + [h for h, _ in splits] + [m for _, m in splits] + [nil]]
    for coord in (x, y):
        for shift in (-1.0, 0.0, 1.0):
            moved = jnp.where(live, coord + shift, 0.0)
            splits = [split2(moved)] + [split2(part * moved) for part in parts]
            groups.append([h for h, _ in splits] + [m for _, m in splits])
    put_rows(ref, at, [row for group in groups for row in group], width)


def remote(src, dst, send, recv, to_x, to_y):
    return pltpu.make_async_remote_copy(
        src_ref=src,
        dst_ref=dst,
        send_sem=send,
        recv_sem=recv,
        device_id=(to_x, to_y),
        device_id_type=pl.DeviceIdType.MESH,
    )


def step_kernel(
    nx, ny,
    pos_in, vel_in, oth_in, code_in,
    pos_out, vel_out, press_out, bounds_out,
    base, pos, acc, press, parts, ratio, dens, dsum,
    jf, jfh, lhs, xf, yf, af, vf, vfh, sums, gram,
    pos_pack, pos_row, pos_col, pos_cor, ab_pack, ab_row, ab_col, ab_cor,
    red_snd, red_rcv,
    pos_ss, pos_rs, ab_ss, ab_rs, red_ss, red_rs,
):
    _, rows, cols, slots = pos_in.shape
    width, half = cols + 2, cols // 2
    others = nx * ny - 1
    me_x, me_y = lax.axis_index("gx"), lax.axis_index("gy")

    def at_x(step):
        return lax.rem(me_x + step + nx, nx)

    def at_y(step):
        return lax.rem(me_y + step + ny, ny)

    for ref in (pos_row, pos_col, pos_cor, ab_row, ab_col, ab_cor):
        ref[...] = jnp.zeros_like(ref)
    peers = [(dx, dy) for dx in range(nx) for dy in range(ny) if dx or dy]
    barrier = pltpu.get_barrier_semaphore()
    for dx, dy in peers:
        pl.semaphore_signal(
            barrier, inc=1, device_id=(at_x(dx), at_y(dy)), device_id_type=pl.DeviceIdType.MESH
        )

    for ref in (base, acc, press, pos, dens, ratio, parts, sums, pos_pack, ab_pack):
        ref[...] = jnp.zeros_like(ref)
    like = jnp.zeros((width, slots), jnp.float32)
    for row in range(rows):
        for k, source in enumerate((pos_in, vel_in, oth_in)):
            for c in range(2):
                base[2 * k + c, row, 1 : cols + 1, :] = source[c, row]
        base[6, row, 1 : cols + 1, :] = code_in[row]
        target_constants(xf, yf, af, row, width, like)
    for row in range(rows + 2):
        source_constants(jf, row, width, like)
    for at in range(3):
        source_constants(jfh, at, 8, jnp.zeros((8, slots), jnp.float32))
    pl.semaphore_wait(barrier, others)

    def halo(field, pack, row_got, col_got, cor_got, send, recv, par):
        copies = []
        for d, (dx, dy) in enumerate(DIRS):
            row = rows - 1 if dx > 0 else 0
            side_x, side_y = (0 if dx > 0 else 1), (0 if dy > 0 else 1)
            if dy == 0:
                src, dst = field.at[:, row], row_got.at[par, side_x]
            elif dx == 0:
                src = pack.at[1 - side_y, :, pl.ds(0, rows)]
                dst = col_got.at[par, side_y, :, pl.ds(0, rows)]
            else:
                src = pack.at[1 - side_y, :, pl.ds(row, 1)]
                dst = cor_got.at[par, :, pl.ds(2 * side_x + side_y, 1)]
            copies.append(remote(src, dst, send.at[par, d], recv.at[par, d], at_x(dx), at_y(dy)))
        return copies

    def pack_columns(field, pack, count):
        for k in range(count):
            for side, cell in enumerate((1, cols)):
                for r in range(rows):
                    pack[side, k, r : r + 1, :] = field[k, r, cell : cell + 1, :]

    def cell_rows(inner, outer, srow, col, pick):
        if 1 <= col <= cols:
            return inner[srow, pick(col, width), :]
        side = 0 if col == 0 else 1
        if srow in (0, rows + 1):
            return outer[2, pick(2 * (0 if srow == 0 else 1) + side, 8), :]
        return outer[side, pick(srow - 1, 8), :]

    def build_lhs(srow, q):
        def pick(at, step):
            return pl.ds(at, 24, stride=step)

        both = jnp.concatenate(
            [
                cell_rows(jf, jfh, srow, q, pick),
                cell_rows(jf, jfh, srow, width - 1 - q, pick),
            ],
            axis=0,
        )
        lhs[srow, q] = both.T.astype(jnp.bfloat16)

    def target_block(row, cell, ax, ay):
        at = pl.ds(cell, 8, stride=width)
        return jnp.concatenate(
            [xf[row, ax, at, :], yf[row, ay, at, :], af[row, 3 * ax + ay, at, :]], axis=0
        )

    def density_block(row, p, ax, ay):
        first = target_block(row, p + 1, ax, ay)
        second = target_block(row, cols - p, ax, 2 - ay)
        nil = jnp.zeros_like(first)
        rhs = jnp.concatenate(
            [
                jnp.concatenate([first, nil], axis=1),
                jnp.concatenate([nil, second], axis=1),
            ],
            axis=0,
        ).astype(jnp.bfloat16)
        raw = jnp.dot(lhs[row + ax, p + ay], rhs, preferred_element_type=jnp.float32)
        w = jnp.maximum(raw, 0.0)
        square = w * w
        gram[row, p, 3 * ax + ay] = square
        return jnp.sum((square * w).reshape(slots // 8, 8, 2 * slots), axis=0)

    def density_blocks(row, p, blocks, fresh):
        total = None if fresh else dsum[row, p]
        for ax, ay in blocks:
            got = density_block(row, p, ax, ay)
            total = got if total is None else total + got
        dsum[row, p] = total

    def value_cell(srow, col, ax, ay):
        def pick(group):
            return lambda at, step: pl.ds(8 * step * group + at, 8, stride=step)

        return [
            cell_rows(vf, vfh, srow, col, pick(group)) for group in (0, 1 + ax, 4 + ay)
        ]

    def force_blocks(row, p, blocks, fresh):
        left, high, low = [], [], []
        for ax, ay in blocks:
            q = p + ay
            left.append(
                jnp.concatenate(
                    value_cell(row + ax, q, ax, ay)
                    + value_cell(row + ax, width - 1 - q, ax, 2 - ay),
                    axis=0,
                ).astype(jnp.bfloat16)
            )
            g = gram[row, p, 3 * ax + ay]
            h = g.astype(jnp.bfloat16)
            high.append(h)
            low.append((g - h.astype(jnp.float32)).astype(jnp.bfloat16))
        got = jnp.dot(
            jnp.concatenate(left + left, axis=1),
            jnp.concatenate(high + low, axis=0),
            preferred_element_type=jnp.float32,
        )
        for col, piece in ((p + 1, got[:24, :slots]), (cols - p, got[24:, slots:])):
            at = pl.ds(col, 24, stride=width)
            sums[row, at, :] = piece if fresh else sums[row, at, :] + piece

    every = [(ax, ay) for ax in range(3) for ay in range(3)]

    def inner_blocks(row, p):
        return [
            (ax, ay)
            for ax, ay in every
            if 1 <= row + ax <= rows and 1 <= p + ay <= cols
        ]

    def inner_phase(blocks_of):
        def middle(step, carry):
            for k in range(2):
                for p in range(half):
                    blocks_of(1 + 2 * step + k, p, inner_blocks(1, p), True)
            return carry

        pairs = (rows - 2) // 2
        lax.fori_loop(0, pairs, middle, 0)
        for row in [0] + list(range(1 + 2 * pairs, rows)):
            for p in range(half):
                blocks_of(row, p, inner_blocks(row, p), True)

    def outer_phase(blocks_of, corners):
        for row in range(rows):
            for p in range(half):
                inner = inner_blocks(row, p)
                blocks = [
                    (ax, ay)
                    for ax, ay in every
                    if (ax, ay) not in inner
                    and (row + ax in (0, rows + 1) and p + ay == 0) == corners
                ]
                if blocks:
                    blocks_of(row, p, blocks, False)

    def one_iteration(it, carry):
        par = lax.rem(it, 2)

        for row in range(rows):
            live = base[6, row] > 0
            for c in range(2):
                vel = base[2 + c, row] + TIME_STEP * (base[4 + c, row] + acc[c, row])
                moved = base[c, row] + TIME_STEP * vel
                pos[c, row] = jnp.where(live, moved, FAR if c == 0 else 0.0)
        pack_columns(pos, pos_pack, 2)
        pos_copies = halo(pos, pos_pack, pos_row, pos_col, pos_cor, pos_ss, pos_rs, par)
        for copy in pos_copies:
            copy.start()

        for row in range(rows):
            source_features(pos[0, row], pos[1, row], jf, row + 1, width)
            for q in range(1, half + 2):
                build_lhs(row + 1, q)
        for row in range(rows):
            target_features(pos[0, row], pos[1, row], xf, yf, af, row, width)
        inner_phase(density_blocks)

        for copy in pos_copies[4:]:
            copy.wait_recv()
        for side, srow in enumerate((0, rows + 1)):
            source_features(pos_row[par, side, 0], pos_row[par, side, 1], jf, srow, width)
            source_features(pos_col[par, side, 0], pos_col[par, side, 1], jfh, side, 8)
            for q in range(1, half + 2):
                build_lhs(srow, q)
        for row in range(rows):
            build_lhs(row + 1, 0)
        outer_phase(density_blocks, False)

        for copy in pos_copies[:4]:
            copy.wait_recv()
        source_features(pos_cor[par, 0], pos_cor[par, 1], jfh, 2, 8)
        for srow in (0, rows + 1):
            build_lhs(srow, 0)
        outer_phase(density_blocks, True)

        best = [jnp.full((width, slots), -SENTINEL, jnp.float32)] * 4
        for row in range(rows):
            for p in range(half):
                got = jnp.sum(dsum[row, p], axis=0, keepdims=True)
                dens[row, p + 1 : p + 2, :] = got[:, :slots]
                dens[row, cols - p : cols - p + 1, :] = got[:, slots:]
        for row in range(rows):
            code = base[6, row]
            live = code > 0.5
            heavy = code > 1.5
            density = KERNEL_NORM * dens[row]
            own = density / jnp.where(heavy, REST_HEAVY, REST_LIGHT)
            ratio[row] = own
            light_sel = live & jnp.logical_not(heavy)
            heavy_sel = live & heavy
            for k, (sel, value) in enumerate(
                ((light_sel, own), (heavy_sel, own), (light_sel, -own), (heavy_sel, -own))
            ):
                best[k] = jnp.maximum(best[k], jnp.where(sel, value, -SENTINEL))
        lane = lax.broadcasted_iota(jnp.int32, (1, slots), 1)
        mine = jnp.full((1, slots), -SENTINEL, jnp.float32)
        for k in range(4):
            peak = jnp.max(jnp.max(best[k], axis=0, keepdims=True), axis=1, keepdims=True)
            mine = jnp.where(lane == k, peak, mine)
        red_snd[par] = mine
        for k, (dx, dy) in enumerate(peers):
            remote(
                red_snd.at[par],
                red_rcv.at[par, pl.ds(k, 1)],
                red_ss.at[par],
                red_rs.at[par],
                at_x(dx),
                at_y(dy),
            ).start()

        for row in range(rows):
            code = base[6, row]
            live = code > 0.5
            heavy = code > 1.5
            own = ratio[row]
            density = KERNEL_NORM * dens[row]
            safe = jnp.where(live, density, 1.0)
            scale = 1.0 / (safe * safe)
            stiff = jnp.where(heavy, STIFF_HEAVY, STIFF_LIGHT)
            beta = jnp.where(live, stiff * (own - 1.0) * scale, 0.0)
            parts[0, row] = jnp.where(live, press[row] * scale, 0.0)
            parts[1, row] = jnp.where(heavy, 0.0, beta)
            parts[2, row] = jnp.where(heavy, beta, 0.0)
        pack_columns(parts, ab_pack, 3)
        ab_copies = halo(parts, ab_pack, ab_row, ab_col, ab_cor, ab_ss, ab_rs, par)
        for copy in ab_copies:
            copy.start()

        for row in range(rows):
            value_rows(
                pos[0, row], pos[1, row], [parts[k, row] for k in range(3)], vf, row + 1, width
            )
        inner_phase(force_blocks)

        for copy in ab_copies[4:]:
            copy.wait_recv()
        for side, srow in enumerate((0, rows + 1)):
            value_rows(
                pos_row[par, side, 0], pos_row[par, side, 1],
                [ab_row[par, side, k] for k in range(3)], vf, srow, width,
            )
            value_rows(
                pos_col[par, side, 0], pos_col[par, side, 1],
                [ab_col[par, side, k] for k in range(3)], vfh, side, 8,
            )
        outer_phase(force_blocks, False)
        for copy in ab_copies[:4]:
            copy.wait_recv()
        value_rows(
            pos_cor[par, 0], pos_cor[par, 1], [ab_cor[par, k] for k in range(3)], vfh, 2, 8
        )
        outer_phase(force_blocks, True)

        for copy in pos_copies + ab_copies:
            copy.wait_send()
        everyone = red_rcv.at[par, pl.ds(0, others)]
        pltpu.make_async_copy(everyone, everyone, red_ss.at[par]).wait()
        pltpu.make_async_copy(everyone, everyone, red_rs.at[par]).wait()
        top = jnp.maximum(
            red_snd[par], jnp.max(red_rcv[par, 0:others, :], axis=0, keepdims=True)
        )
        bound = [
            jnp.max(jnp.where(lane == k, top, -SENTINEL), axis=1, keepdims=True)
            for k in range(4)
        ]
        bounds_out[it] = jnp.where(lane < 2, top, -top)
        relax_light = 1.0 / (1.0 + bound[0] + bound[2])
        relax_heavy = 1.0 / (1.0 + bound[1] + bound[3])

        for row in range(rows):
            def total(k):
                return sums[row, k * width : (k + 1) * width, :]

            def linear(k, mid):
                return (
                    (total(k) + total(k + mid))
                    + relax_light * (total(k + 1) + total(k + 1 + mid))
                    + relax_heavy * (total(k + 2) + total(k + 2 + mid))
                )

            code = base[6, row]
            live = code > 0.5
            heavy = code > 1.5
            relaxed = jnp.where(heavy, STIFF_HEAVY * relax_heavy, STIFF_LIGHT * relax_light)
            press[row] = jnp.where(live, press[row] + relaxed * (ratio[row] - 1.0), 0.0)
            term = parts[0, row] + relax_light * parts[1, row] + relax_heavy * parts[2, row]
            scale = jnp.where(
                heavy, 6.0 * KERNEL_NORM / MASS_HEAVY, 6.0 * KERNEL_NORM / MASS_LIGHT
            )
            plain, by_term = total(0), linear(1, 3)
            for c in range(2):
                own = pos[c, row] - 0.5
                first = 8 + 8 * c
                placed = total(first) + total(first + 4)
                force = term * (own * plain - placed) + own * by_term - linear(first + 1, 4)
                acc[c, row] = jnp.where(live, scale * force, 0.0)
        return carry

    lax.fori_loop(0, ITERS, one_iteration, 0)

    for row in range(rows):
        live = base[6, row] > 0.5
        press_out[row] = press[row, 1 : cols + 1, :]
        for c in range(2):
            vel = base[2 + c, row] + TIME_STEP * (base[4 + c, row] + acc[c, row])
            vel = jnp.where(live, vel, 0.0)
            place = jnp.where(live, base[c, row] + TIME_STEP * vel, 0.0)
            vel_out[c, row] = vel[1 : cols + 1]
            pos_out[c, row] = place[1 : cols + 1]


def local(position, velocity, other_accel, phase_ids, counts):
    rows, cols, slots = phase_ids.shape
    width, half = cols + 2, cols // 2
    nx, ny = lax.axis_size("gx"), lax.axis_size("gy")
    tall = -(-rows // 8) * 8
    slot_index = jnp.arange(slots, dtype=jnp.int32)
    live = slot_index[None, None, :] < counts[:, :, None]
    codes = jnp.where(live, phase_ids + 1, 0).astype(jnp.float32)

    def vm(*shape):
        return pltpu.VMEM(shape, jnp.float32)

    dma = pltpu.SemaphoreType.DMA
    new_pos, new_vel, pressure, bounds = pl.pallas_call(
        functools.partial(step_kernel, nx, ny),
        out_shape=(
            jax.ShapeDtypeStruct((2, rows, cols, slots), jnp.float32),
            jax.ShapeDtypeStruct((2, rows, cols, slots), jnp.float32),
            jax.ShapeDtypeStruct((rows, cols, slots), jnp.float32),
            jax.ShapeDtypeStruct((ITERS, 1, slots), jnp.float32),
        ),
        in_specs=[pl.BlockSpec(memory_space=pltpu.VMEM)] * 4,
        out_specs=(pl.BlockSpec(memory_space=pltpu.VMEM),) * 4,
        scratch_shapes=[
            vm(7, rows, width, slots),
            vm(2, rows, width, slots),
            vm(2, rows, width, slots),
            vm(rows, width, slots),
            vm(3, rows, width, slots),
            vm(rows, width, slots),
            vm(rows, width, slots),
            vm(rows, half, 8, 2 * slots),
            vm(rows + 2, 24 * width, slots),
            vm(3, 24 * tall, slots),
            pltpu.VMEM((rows + 2, half + 2, slots, 48), jnp.bfloat16),
            vm(rows, 3, 8 * width, slots),
            vm(rows, 3, 8 * width, slots),
            vm(rows, 9, 8 * width, slots),
            vm(rows + 2, 56 * width, slots),
            vm(3, 56 * tall, slots),
            vm(rows, 24 * width, slots),
            vm(rows, half, 9, slots, 2 * slots),
            vm(2, 2, tall, slots),
            vm(2, 2, 2, width, slots),
            vm(2, 2, 2, tall, slots),
            vm(2, 2, tall, slots),
            vm(2, 3, tall, slots),
            vm(2, 2, 3, width, slots),
            vm(2, 2, 3, tall, slots),
            vm(2, 3, tall, slots),
            vm(2, 1, slots),
            vm(2, nx * ny, slots),
            dma((2, 8)), dma((2, 8)), dma((2, 8)), dma((2, 8)), dma((2,)), dma((2,)),
        ],
        compiler_params=pltpu.CompilerParams(collective_id=0, has_side_effects=True),
    )(position, velocity, other_accel, codes)
    return new_pos, new_vel, pressure, bounds[:, 0, :4]


def solution(mesh):
    placed = (
        P(None, "gx", "gy", None),
        P(None, "gx", "gy", None),
        P(None, "gx", "gy", None),
        P("gx", "gy", None),
        P("gx", "gy"),
    )
    return jax.shard_map(
        local,
        mesh=mesh,
        in_specs=placed,
        out_specs=(P(None, "gx", "gy", None), P(None, "gx", "gy", None), P("gx", "gy", None), P()),
        check_vma=False,
    )
```

```python
import functools

import jax
import jax.numpy as jnp
from jax import lax
from jax.experimental import pallas as pl
from jax.experimental.pallas import tpu as pltpu
from jax.sharding import PartitionSpec as P

ITERS = 4


TIME_STEP = 0.05
KERNEL_NORM = 4.0 / (3.141592653589793 * 64.0)
REST_LIGHT = 1.2
REST_HEAVY = 1.5
STIFF_LIGHT = 100.0
STIFF_HEAVY = 200.0
MASS_LIGHT = 1.0
MASS_HEAVY = 1.5
SENTINEL = 1e30


EMPTY = -1e30
FAR = 1e30
LIMIT = 1e29
DIAGONALS = tuple((dx, dy) for dx in (-1, 1) for dy in (-1, 1))
SIDES = ((-1, 0), (1, 0), (0, -1), (0, 1))
DIRS = DIAGONALS + SIDES


def rounded(value):
    return value.astype(jnp.bfloat16).astype(jnp.float32)


def split2(value):
    high = rounded(value)
    return high, rounded(value - high)


def split3(value):
    high = rounded(value)
    rest = value - high
    mid = rounded(rest)
    return high, mid, rounded(rest - mid)


def put_rows(ref, at, values, width):
    for k, value in enumerate(values):
        ref[at, k * width : (k + 1) * width, :] = value


def source_features(x, y, ref, at, width):
    live = x < LIMIT
    x = jnp.where(live, x - 0.5, 0.0)
    y = jnp.where(live, y - 0.5, 0.0)
    xh, xm, xl = split3(x)
    yh, ym, yl = split3(y)
    bh, bm, bl = split3(jnp.where(live, -(x * x + y * y), EMPTY))
    put_rows(
        ref,
        at,
        [xh, xh, xm, xh, xl, xm, bh, bm, yh, yh, ym, yh, yl, ym, bl],
        width,
    )


def source_constants(ref, at, width, like):
    nil, one = jnp.zeros_like(like), jnp.ones_like(like)
    for k in range(15, 24):
        ref[at, k * width : (k + 1) * width, :] = one if 16 <= k <= 18 else nil


def target_features(x, y, xf, yf, af, row, width):
    x = jnp.where(x < LIMIT, x, 0.0) - 0.5
    y = y - 0.5
    for at in range(3):
        h, m, l = split3(2.0 * (x - (at - 1.0)))
        put_rows(xf.at[row], at, [h, m, h, l, h, m], width)
        h, m, l = split3(2.0 * (y - (at - 1.0)))
        put_rows(yf.at[row], at, [h, m, h, l, h, m], width)
    for ax in range(3):
        for ay in range(3):
            dx = x - (ax - 1.0)
            dy = y - (ay - 1.0)
            put_rows(af.at[row], 3 * ax + ay, split3(1.0 - (dx * dx + dy * dy)), width)


def target_constants(xf, yf, af, row, width, like):
    nil, one = jnp.zeros_like(like), jnp.ones_like(like)
    for at in range(3):
        for ref, values in ((xf, (one, one)), (yf, (one, nil))):
            for k, value in enumerate(values):
                ref[row, at, (6 + k) * width : (7 + k) * width, :] = value
    for at in range(9):
        for k in range(3, 8):
            af[row, at, k * width : (k + 1) * width, :] = nil


def value_rows(x, y, parts, ref, at, width):
    live = x < LIMIT
    x = jnp.where(live, x - 0.5, 0.0)
    y = jnp.where(live, y - 0.5, 0.0)
    parts = [jnp.where(live, part, 0.0) for part in parts]
    splits = [split2(part) for part in parts]
    one = jnp.where(live, 1.0, 0.0)
    nil = jnp.zeros_like(x)
    groups = [[one] + [h for h, _ in splits] + [m for _, m in splits] + [nil]]
    for coord in (x, y):
        for shift in (-1.0, 0.0, 1.0):
            moved = jnp.where(live, coord + shift, 0.0)
            splits = [split2(moved)] + [split2(part * moved) for part in parts]
            groups.append([h for h, _ in splits] + [m for _, m in splits])
    put_rows(ref, at, [row for group in groups for row in group], width)


def remote(src, dst, send, recv, to_x, to_y):
    return pltpu.make_async_remote_copy(
        src_ref=src,
        dst_ref=dst,
        send_sem=send,
        recv_sem=recv,
        device_id=(to_x, to_y),
        device_id_type=pl.DeviceIdType.MESH,
    )


def step_kernel(
    nx, ny,
    pos_in, vel_in, oth_in, phase_in, counts_in,
    pos_out, vel_out, press_out, bounds_out,
    phases, counts, in_sem,
    base, pos, acc, press, parts, ratio, dens, dsum,
    jf, jfh, lhs, xf, yf, af, vf, vfh, sums, gram,
    pos_pack, pos_row, pos_col, pos_cor, ab_pack, ab_row, ab_col, ab_cor,
    red_snd, red_rcv,
    pos_ss, pos_rs, ab_ss, ab_rs, red_ss, red_rs,
):
    rows, cols, _, slots = pos_in.shape
    width, half = cols + 2, cols // 2
    others = nx * ny - 1
    me_x, me_y = lax.axis_index("gx"), lax.axis_index("gy")

    def at_x(step):
        return lax.rem(me_x + step + nx, nx)

    def at_y(step):
        return lax.rem(me_y + step + ny, ny)

    for k in range(6):
        for row in range(rows):
            for cell in (0, width - 1):
                base[k, row, cell : cell + 1, :] = jnp.zeros((1, slots), jnp.float32)
    loads = [
        pltpu.make_async_copy(phase_in, phases, in_sem.at[6]),
        pltpu.make_async_copy(counts_in, counts, in_sem.at[7]),
    ]
    for k, source in enumerate((pos_in, vel_in, oth_in)):
        for c in range(2):
            loads.append(
                pltpu.make_async_copy(
                    source.at[:, :, c],
                    base.at[2 * k + c, :, pl.ds(1, cols)],
                    in_sem.at[2 * k + c],
                )
            )
    for copy in loads:
        copy.start()
    for ref in (pos_row, pos_col, pos_cor, ab_row, ab_col, ab_cor):
        ref[...] = jnp.zeros_like(ref)
    peers = [(dx, dy) for dx in range(nx) for dy in range(ny) if dx or dy]
    barrier = pltpu.get_barrier_semaphore()
    for dx, dy in peers:
        pl.semaphore_signal(
            barrier, inc=1, device_id=(at_x(dx), at_y(dy)), device_id_type=pl.DeviceIdType.MESH
        )

    for ref in (acc, press, pos, dens, ratio, parts, sums, pos_pack, ab_pack):
        ref[...] = jnp.zeros_like(ref)
    like = jnp.zeros((width, slots), jnp.float32)
    for row in range(rows):
        base[6, row] = like
        target_constants(xf, yf, af, row, width, like)
    for row in range(rows + 2):
        source_constants(jf, row, width, like)
    for at in range(3):
        source_constants(jfh, at, 8, jnp.zeros((8, slots), jnp.float32))
    for copy in loads:
        copy.wait()
    slot = lax.broadcasted_iota(jnp.int32, (1, slots), 1)
    for row in range(rows):
        for cell in range(cols):
            code = jnp.where(slot < counts[row, cell], phases[row, cell : cell + 1, :] + 1, 0)
            base[6, row, cell + 1 : cell + 2, :] = code.astype(jnp.float32)
    pl.semaphore_wait(barrier, others)

    def halo(field, pack, row_got, col_got, cor_got, send, recv, par):
        copies = []
        for d, (dx, dy) in enumerate(DIRS):
            row = rows - 1 if dx > 0 else 0
            side_x, side_y = (0 if dx > 0 else 1), (0 if dy > 0 else 1)
            if dy == 0:
                src, dst = field.at[:, row], row_got.at[par, side_x]
            elif dx == 0:
                src = pack.at[1 - side_y, :, pl.ds(0, rows)]
                dst = col_got.at[par, side_y, :, pl.ds(0, rows)]
            else:
                src = pack.at[1 - side_y, :, pl.ds(row, 1)]
                dst = cor_got.at[par, :, pl.ds(2 * side_x + side_y, 1)]
            copies.append(remote(src, dst, send.at[par, d], recv.at[par, d], at_x(dx), at_y(dy)))
        return copies

    def pack_columns(field, pack, count):
        for k in range(count):
            for side, cell in enumerate((1, cols)):
                for r in range(rows):
                    pack[side, k, r : r + 1, :] = field[k, r, cell : cell + 1, :]

    def cell_rows(inner, outer, srow, col, pick):
        if 1 <= col <= cols:
            return inner[srow, pick(col, width), :]
        side = 0 if col == 0 else 1
        if srow in (0, rows + 1):
            return outer[2, pick(2 * (0 if srow == 0 else 1) + side, 8), :]
        return outer[side, pick(srow - 1, 8), :]

    def build_lhs(srow, q):
        def pick(at, step):
            return pl.ds(at, 24, stride=step)

        both = jnp.concatenate(
            [
                cell_rows(jf, jfh, srow, q, pick),
                cell_rows(jf, jfh, srow, width - 1 - q, pick),
            ],
            axis=0,
        )
        lhs[srow, q] = both.T.astype(jnp.bfloat16)

    def target_block(row, cell, ax, ay):
        at = pl.ds(cell, 8, stride=width)
        return jnp.concatenate(
            [xf[row, ax, at, :], yf[row, ay, at, :], af[row, 3 * ax + ay, at, :]], axis=0
        )

    def density_block(row, p, ax, ay):
        first = target_block(row, p + 1, ax, ay)
        second = target_block(row, cols - p, ax, 2 - ay)
        nil = jnp.zeros_like(first)
        rhs = jnp.concatenate(
            [
                jnp.concatenate([first, nil], axis=1),
                jnp.concatenate([nil, second], axis=1),
            ],
            axis=0,
        ).astype(jnp.bfloat16)
        raw = jnp.dot(lhs[row + ax, p + ay], rhs, preferred_element_type=jnp.float32)
        w = jnp.maximum(raw, 0.0)
        square = w * w
        gram[row, p, 3 * ax + ay] = square
        return jnp.sum((square * w).reshape(slots // 8, 8, 2 * slots), axis=0)

    def density_blocks(row, p, blocks, fresh):
        total = None if fresh else dsum[row, p]
        for ax, ay in blocks:
            got = density_block(row, p, ax, ay)
            total = got if total is None else total + got
        dsum[row, p] = total

    def value_cell(srow, col, ax, ay):
        def pick(group):
            return lambda at, step: pl.ds(8 * step * group + at, 8, stride=step)

        return [
            cell_rows(vf, vfh, srow, col, pick(group)) for group in (0, 1 + ax, 4 + ay)
        ]

    def force_blocks(row, p, blocks, fresh):
        left, both = [], []
        for ax, ay in blocks:
            q = p + ay
            left.append(
                jnp.concatenate(
                    value_cell(row + ax, q, ax, ay)
                    + value_cell(row + ax, width - 1 - q, ax, 2 - ay),
                    axis=0,
                ).astype(jnp.bfloat16)
            )
            g = gram[row, p, 3 * ax + ay]
            h = g.astype(jnp.bfloat16)
            left.append(left[-1])
            both.append(h)
            both.append((g - h.astype(jnp.float32)).astype(jnp.bfloat16))
        got = jnp.dot(
            jnp.concatenate(left, axis=1),
            jnp.concatenate(both, axis=0),
            preferred_element_type=jnp.float32,
        )
        for col, piece in ((p + 1, got[:24, :slots]), (cols - p, got[24:, slots:])):
            at = pl.ds(col, 24, stride=width)
            sums[row, at, :] = piece if fresh else sums[row, at, :] + piece

    every = [(ax, ay) for ax in range(3) for ay in range(3)]

    def inner_blocks(row, p):
        return [
            (ax, ay)
            for ax, ay in every
            if 1 <= row + ax <= rows and 1 <= p + ay <= cols
        ]

    def inner_phase(blocks_of):
        def middle(step, carry):
            for k in range(2):
                for p in range(half):
                    blocks_of(1 + 2 * step + k, p, inner_blocks(1, p), True)
            return carry

        pairs = (rows - 2) // 2
        lax.fori_loop(0, pairs, middle, 0)
        for row in [0] + list(range(1 + 2 * pairs, rows)):
            for p in range(half):
                blocks_of(row, p, inner_blocks(row, p), True)

    def outer_phase(blocks_of, corners):
        for row in range(rows):
            for p in range(half):
                inner = inner_blocks(row, p)
                blocks = [
                    (ax, ay)
                    for ax, ay in every
                    if (ax, ay) not in inner
                    and (row + ax in (0, rows + 1) and p + ay == 0) == corners
                ]
                if blocks:
                    blocks_of(row, p, blocks, False)

    def one_iteration(it, carry):
        par = lax.rem(it, 2)

        for row in range(rows):
            live = base[6, row] > 0
            for c in range(2):
                vel = base[2 + c, row] + TIME_STEP * (base[4 + c, row] + acc[c, row])
                moved = base[c, row] + TIME_STEP * vel
                pos[c, row] = jnp.where(live, moved, FAR if c == 0 else 0.0)
        pack_columns(pos, pos_pack, 2)
        pos_copies = halo(pos, pos_pack, pos_row, pos_col, pos_cor, pos_ss, pos_rs, par)
        for copy in pos_copies:
            copy.start()

        for row in range(rows):
            source_features(pos[0, row], pos[1, row], jf, row + 1, width)
            for q in range(1, half + 2):
                build_lhs(row + 1, q)
        for row in range(rows):
            target_features(pos[0, row], pos[1, row], xf, yf, af, row, width)
        inner_phase(density_blocks)

        for copy in pos_copies[4:]:
            copy.wait_recv()
        for side, srow in enumerate((0, rows + 1)):
            source_features(pos_row[par, side, 0], pos_row[par, side, 1], jf, srow, width)
            source_features(pos_col[par, side, 0], pos_col[par, side, 1], jfh, side, 8)
            for q in range(1, half + 2):
                build_lhs(srow, q)
        for row in range(rows):
            build_lhs(row + 1, 0)
        outer_phase(density_blocks, False)

        for copy in pos_copies[:4]:
            copy.wait_recv()
        source_features(pos_cor[par, 0], pos_cor[par, 1], jfh, 2, 8)
        for srow in (0, rows + 1):
            build_lhs(srow, 0)
        outer_phase(density_blocks, True)

        best = [jnp.full((width, slots), -SENTINEL, jnp.float32)] * 4
        for row in range(rows):
            for p in range(half):
                got = jnp.sum(dsum[row, p], axis=0, keepdims=True)
                dens[row, p + 1 : p + 2, :] = got[:, :slots]
                dens[row, cols - p : cols - p + 1, :] = got[:, slots:]
        for row in range(rows):
            code = base[6, row]
            live = code > 0.5
            heavy = code > 1.5
            density = KERNEL_NORM * dens[row]
            own = density / jnp.where(heavy, REST_HEAVY, REST_LIGHT)
            ratio[row] = own
            light_sel = live & jnp.logical_not(heavy)
            heavy_sel = live & heavy
            for k, (sel, value) in enumerate(
                ((light_sel, own), (heavy_sel, own), (light_sel, -own), (heavy_sel, -own))
            ):
                best[k] = jnp.maximum(best[k], jnp.where(sel, value, -SENTINEL))
        lane = lax.broadcasted_iota(jnp.int32, (1, slots), 1)
        mine = jnp.full((1, slots), -SENTINEL, jnp.float32)
        for k in range(4):
            peak = jnp.max(jnp.max(best[k], axis=0, keepdims=True), axis=1, keepdims=True)
            mine = jnp.where(lane == k, peak, mine)
        red_snd[par] = mine
        for k, (dx, dy) in enumerate(peers):
            remote(
                red_snd.at[par],
                red_rcv.at[par, pl.ds(k, 1)],
                red_ss.at[par],
                red_rs.at[par],
                at_x(dx),
                at_y(dy),
            ).start()

        for row in range(rows):
            code = base[6, row]
            live = code > 0.5
            heavy = code > 1.5
            own = ratio[row]
            density = KERNEL_NORM * dens[row]
            safe = jnp.where(live, density, 1.0)
            scale = 1.0 / (safe * safe)
            stiff = jnp.where(heavy, STIFF_HEAVY, STIFF_LIGHT)
            beta = jnp.where(live, stiff * (own - 1.0) * scale, 0.0)
            parts[0, row] = jnp.where(live, press[row] * scale, 0.0)
            parts[1, row] = jnp.where(heavy, 0.0, beta)
            parts[2, row] = jnp.where(heavy, beta, 0.0)
        pack_columns(parts, ab_pack, 3)
        ab_copies = halo(parts, ab_pack, ab_row, ab_col, ab_cor, ab_ss, ab_rs, par)
        for copy in ab_copies:
            copy.start()

        for row in range(rows):
            value_rows(
                pos[0, row], pos[1, row], [parts[k, row] for k in range(3)], vf, row + 1, width
            )
        inner_phase(force_blocks)

        for copy in ab_copies[4:]:
            copy.wait_recv()
        for side, srow in enumerate((0, rows + 1)):
            value_rows(
                pos_row[par, side, 0], pos_row[par, side, 1],
                [ab_row[par, side, k] for k in range(3)], vf, srow, width,
            )
            value_rows(
                pos_col[par, side, 0], pos_col[par, side, 1],
                [ab_col[par, side, k] for k in range(3)], vfh, side, 8,
            )
        outer_phase(force_blocks, False)
        for copy in ab_copies[:4]:
            copy.wait_recv()
        value_rows(
            pos_cor[par, 0], pos_cor[par, 1], [ab_cor[par, k] for k in range(3)], vfh, 2, 8
        )
        outer_phase(force_blocks, True)

        for copy in pos_copies + ab_copies:
            copy.wait_send()
        everyone = red_rcv.at[par, pl.ds(0, others)]
        pltpu.make_async_copy(everyone, everyone, red_ss.at[par]).wait()
        pltpu.make_async_copy(everyone, everyone, red_rs.at[par]).wait()
        top = jnp.maximum(
            red_snd[par], jnp.max(red_rcv[par, 0:others, :], axis=0, keepdims=True)
        )
        bound = [
            jnp.max(jnp.where(lane == k, top, -SENTINEL), axis=1, keepdims=True)
            for k in range(4)
        ]
        bounds_out[it] = jnp.where(lane < 2, top, -top)
        relax_light = 1.0 / (1.0 + bound[0] + bound[2])
        relax_heavy = 1.0 / (1.0 + bound[1] + bound[3])

        for row in range(rows):
            def total(k):
                return sums[row, k * width : (k + 1) * width, :]

            def linear(k, mid):
                return (
                    (total(k) + total(k + mid))
                    + relax_light * (total(k + 1) + total(k + 1 + mid))
                    + relax_heavy * (total(k + 2) + total(k + 2 + mid))
                )

            code = base[6, row]
            live = code > 0.5
            heavy = code > 1.5
            relaxed = jnp.where(heavy, STIFF_HEAVY * relax_heavy, STIFF_LIGHT * relax_light)
            press[row] = jnp.where(live, press[row] + relaxed * (ratio[row] - 1.0), 0.0)
            term = parts[0, row] + relax_light * parts[1, row] + relax_heavy * parts[2, row]
            scale = jnp.where(
                heavy, 6.0 * KERNEL_NORM / MASS_HEAVY, 6.0 * KERNEL_NORM / MASS_LIGHT
            )
            plain, by_term = total(0), linear(1, 3)
            for c in range(2):
                own = pos[c, row] - 0.5
                first = 8 + 8 * c
                placed = total(first) + total(first + 4)
                force = term * (own * plain - placed) + own * by_term - linear(first + 1, 4)
                acc[c, row] = jnp.where(live, scale * force, 0.0)
        return carry

    lax.fori_loop(0, ITERS, one_iteration, 0)

    for row in range(rows):
        live = base[6, row] > 0.5
        press_out[row] = press[row]
        for c in range(2):
            vel = base[2 + c, row] + TIME_STEP * (base[4 + c, row] + acc[c, row])
            vel = jnp.where(live, vel, 0.0)
            vel_out[c, row] = vel
            pos_out[c, row] = jnp.where(live, base[c, row] + TIME_STEP * vel, 0.0)


def deliver_kernel(
    pos_in, vel_in, press_in, bounds_in, pos_out, vel_out, press_out, bounds_out, sem
):
    cols = press_out.shape[1]
    stores = [
        (press_in.at[:, pl.ds(1, cols)], press_out),
        (bounds_in, bounds_out),
    ]
    for source, target in ((pos_in, pos_out), (vel_in, vel_out)):
        for c in range(2):
            stores.append((source.at[c, :, pl.ds(1, cols)], target.at[:, :, c]))
    copies = [
        pltpu.make_async_copy(source, target, sem.at[k])
        for k, (source, target) in enumerate(stores)
    ]
    for copy in copies:
        copy.start()
    for copy in copies:
        copy.wait()


def cell_major(field):
    return jnp.transpose(field, (1, 2, 0, 3))


def slot_major(field):
    return jnp.transpose(field, (2, 0, 1, 3))


def local(position, velocity, other_accel, phase_ids, counts):
    rows, cols, slots = phase_ids.shape
    width, half = cols + 2, cols // 2
    nx, ny = lax.axis_size("gx"), lax.axis_size("gy")
    tall = -(-rows // 8) * 8
    def vm(*shape):
        return pltpu.VMEM(shape, jnp.float32)

    dma = pltpu.SemaphoreType.DMA
    held = pl.pallas_call(
        functools.partial(step_kernel, nx, ny),
        out_shape=(
            pltpu.VMEM((2, rows, width, slots), jnp.float32),
            pltpu.VMEM((2, rows, width, slots), jnp.float32),
            pltpu.VMEM((rows, width, slots), jnp.float32),
            pltpu.VMEM((ITERS, 1, slots), jnp.float32),
        ),
        in_specs=[pl.BlockSpec(memory_space=pltpu.HBM)] * 5,
        out_specs=(pl.BlockSpec(memory_space=pltpu.VMEM),) * 4,
        scratch_shapes=[
            pltpu.VMEM((rows, cols, slots), jnp.int32),
            pltpu.SMEM((rows, cols), jnp.int32),
            dma((8,)),
            vm(7, rows, width, slots),
            vm(2, rows, width, slots),
            vm(2, rows, width, slots),
            vm(rows, width, slots),
            vm(3, rows, width, slots),
            vm(rows, width, slots),
            vm(rows, width, slots),
            vm(rows, half, 8, 2 * slots),
            vm(rows + 2, 24 * width, slots),
            vm(3, 24 * tall, slots),
            pltpu.VMEM((rows + 2, half + 2, slots, 48), jnp.bfloat16),
            vm(rows, 3, 8 * width, slots),
            vm(rows, 3, 8 * width, slots),
            vm(rows, 9, 8 * width, slots),
            vm(rows + 2, 56 * width, slots),
            vm(3, 56 * tall, slots),
            vm(rows, 24 * width, slots),
            vm(rows, half, 9, slots, 2 * slots),
            vm(2, 2, tall, slots),
            vm(2, 2, 2, width, slots),
            vm(2, 2, 2, tall, slots),
            vm(2, 2, tall, slots),
            vm(2, 3, tall, slots),
            vm(2, 2, 3, width, slots),
            vm(2, 2, 3, tall, slots),
            vm(2, 3, tall, slots),
            vm(2, 1, slots),
            vm(2, nx * ny, slots),
            dma((2, 8)), dma((2, 8)), dma((2, 8)), dma((2, 8)), dma((2,)), dma((2,)),
        ],
        compiler_params=pltpu.CompilerParams(collective_id=0, has_side_effects=True, vmem_limit_bytes=40 * 2**20),
    )(*[pltpu.with_memory_space_constraint(v, pltpu.HBM) for v in (cell_major(position), cell_major(velocity), cell_major(other_accel), phase_ids, counts)])
    new_pos, new_vel, pressure, bounds = pl.pallas_call(
        deliver_kernel,
        out_shape=(
            jax.ShapeDtypeStruct((rows, cols, 2, slots), jnp.float32),
            jax.ShapeDtypeStruct((rows, cols, 2, slots), jnp.float32),
            jax.ShapeDtypeStruct((rows, cols, slots), jnp.float32),
            jax.ShapeDtypeStruct((ITERS, 1, slots), jnp.float32),
        ),
        in_specs=[pl.BlockSpec(memory_space=pl.ANY)] * 4,
        out_specs=(pl.BlockSpec(memory_space=pl.ANY),) * 4,
        scratch_shapes=[dma((6,))],
        compiler_params=pltpu.CompilerParams(vmem_limit_bytes=2**20),
    )(*held)
    return slot_major(new_pos), slot_major(new_vel), pressure, bounds[:, 0, :4]


def solution(mesh):
    placed = (
        P(None, "gx", "gy", None),
        P(None, "gx", "gy", None),
        P(None, "gx", "gy", None),
        P("gx", "gy", None),
        P("gx", "gy"),
    )
    return jax.shard_map(
        local,
        mesh=mesh,
        in_specs=placed,
        out_specs=(P(None, "gx", "gy", None), P(None, "gx", "gy", None), P("gx", "gy", None), P()),
        check_vma=False,
    )
```

```python
import functools

import jax
import jax.numpy as jnp
from jax import lax
from jax.experimental import pallas as pl
from jax.experimental.pallas import tpu as pltpu
from jax.sharding import PartitionSpec as P

ITERS = 4


TIME_STEP = 0.05
KERNEL_NORM = 4.0 / (3.141592653589793 * 64.0)
REST_LIGHT = 1.2
REST_HEAVY = 1.5
STIFF_LIGHT = 100.0
STIFF_HEAVY = 200.0
MASS_LIGHT = 1.0
MASS_HEAVY = 1.5
SENTINEL = 1e30


EMPTY = -1e30
FAR = 1e30
LIMIT = 1e29
DIAGONALS = tuple((dx, dy) for dx in (-1, 1) for dy in (-1, 1))
SIDES = ((-1, 0), (1, 0), (0, -1), (0, 1))
DIRS = DIAGONALS + SIDES


def rounded(value):
    return value.astype(jnp.bfloat16).astype(jnp.float32)


def split2(value):
    high = rounded(value)
    return high, rounded(value - high)


def split3(value):
    high = rounded(value)
    rest = value - high
    mid = rounded(rest)
    return high, mid, rounded(rest - mid)


def put_rows(ref, at, values, width):
    for k, value in enumerate(values):
        ref[at, k * width : (k + 1) * width, :] = value


def source_features(x, y, ref, at, width):
    live = x < LIMIT
    x = jnp.where(live, x - 0.5, 0.0)
    y = jnp.where(live, y - 0.5, 0.0)
    xh, xm, xl = split3(x)
    yh, ym, yl = split3(y)
    bh, bm, bl = split3(jnp.where(live, -(x * x + y * y), EMPTY))
    put_rows(
        ref,
        at,
        [xh, xh, xm, xh, xl, xm, bh, bm, yh, yh, ym, yh, yl, ym, bl],
        width,
    )


def source_constants(ref, at, width, like):
    nil, one = jnp.zeros_like(like), jnp.ones_like(like)
    for k in range(15, 24):
        ref[at, k * width : (k + 1) * width, :] = one if 16 <= k <= 18 else nil


def target_features(x, y, xf, yf, af, row, width):
    x = jnp.where(x < LIMIT, x, 0.0) - 0.5
    y = y - 0.5
    for at in range(3):
        h, m, l = split3(2.0 * (x - (at - 1.0)))
        put_rows(xf.at[row], at, [h, m, h, l, h, m], width)
        h, m, l = split3(2.0 * (y - (at - 1.0)))
        put_rows(yf.at[row], at, [h, m, h, l, h, m], width)
    for ax in range(3):
        for ay in range(3):
            dx = x - (ax - 1.0)
            dy = y - (ay - 1.0)
            put_rows(af.at[row], 3 * ax + ay, split3(1.0 - (dx * dx + dy * dy)), width)


def target_constants(xf, yf, af, row, width, like):
    nil, one = jnp.zeros_like(like), jnp.ones_like(like)
    for at in range(3):
        for ref, values in ((xf, (one, one)), (yf, (one, nil))):
            for k, value in enumerate(values):
                ref[row, at, (6 + k) * width : (7 + k) * width, :] = value
    for at in range(9):
        for k in range(3, 8):
            af[row, at, k * width : (k + 1) * width, :] = nil


def value_rows(x, y, parts, ref, at, width):
    live = x < LIMIT
    x = jnp.where(live, x - 0.5, 0.0)
    y = jnp.where(live, y - 0.5, 0.0)
    parts = [jnp.where(live, part, 0.0) for part in parts]
    splits = [split2(part) for part in parts]
    one = jnp.where(live, 1.0, 0.0)
    nil = jnp.zeros_like(x)
    groups = [[one] + [h for h, _ in splits] + [m for _, m in splits] + [nil]]
    for coord in (x, y):
        for shift in (-1.0, 0.0, 1.0):
            moved = jnp.where(live, coord + shift, 0.0)
            splits = [split2(moved)] + [split2(part * moved) for part in parts]
            groups.append([h for h, _ in splits] + [m for _, m in splits])
    put_rows(ref, at, [row for group in groups for row in group], width)


def remote(src, dst, send, recv, to_x, to_y):
    return pltpu.make_async_remote_copy(
        src_ref=src,
        dst_ref=dst,
        send_sem=send,
        recv_sem=recv,
        device_id=(to_x, to_y),
        device_id_type=pl.DeviceIdType.MESH,
    )


def step_kernel(
    nx, ny,
    pos_in, vel_in, oth_in, phase_in, counts_in,
    pos_out, vel_out, press_out, bounds_out,
    phases, counts, in_sem,
    base, pos, acc, press, parts, ratio, dens, dsum,
    jf, jfh, lhs, xf, yf, af, vf, vfh, sums, gram,
    pos_pack, pos_row, pos_col, pos_cor, ab_pack, ab_row, ab_col, ab_cor,
    red_snd, red_rcv,
    pos_ss, pos_rs, ab_ss, ab_rs, red_ss, red_rs,
):
    rows, cols, _, slots = pos_in.shape
    width, half = cols + 2, cols // 2
    others = nx * ny - 1
    me_x, me_y = lax.axis_index("gx"), lax.axis_index("gy")

    def wrapped(at, size):
        at = jnp.where(at < 0, at + size, at)
        return jnp.where(at >= size, at - size, at)

    def at_x(step):
        return wrapped(me_x + step, nx)

    def at_y(step):
        return wrapped(me_y + step, ny)

    for ref in (pos_row, pos_col, pos_cor, ab_row, ab_col, ab_cor):
        ref[...] = jnp.zeros_like(ref)
    peers = [(dx, dy) for dx in range(nx) for dy in range(ny) if dx or dy]
    barrier = pltpu.get_barrier_semaphore()
    for dx, dy in peers:
        pl.semaphore_signal(
            barrier, inc=1, device_id=(at_x(dx), at_y(dy)), device_id_type=pl.DeviceIdType.MESH
        )

    for k in range(6):
        for row in range(rows):
            for cell in (0, width - 1):
                base[k, row, cell : cell + 1, :] = jnp.zeros((1, slots), jnp.float32)
    loads = [
        pltpu.make_async_copy(phase_in, phases, in_sem.at[6]),
        pltpu.make_async_copy(counts_in, counts, in_sem.at[7]),
    ]
    for k, source in enumerate((pos_in, vel_in, oth_in)):
        for c in range(2):
            loads.append(
                pltpu.make_async_copy(
                    source.at[:, :, c],
                    base.at[2 * k + c, :, pl.ds(1, cols)],
                    in_sem.at[2 * k + c],
                )
            )
    for copy in loads:
        copy.start()
    for ref in (acc, press, pos, dens, ratio, parts, sums, pos_pack, ab_pack):
        ref[...] = jnp.zeros_like(ref)
    like = jnp.zeros((width, slots), jnp.float32)
    for row in range(rows):
        base[6, row] = like
        target_constants(xf, yf, af, row, width, like)
    for row in range(rows + 2):
        source_constants(jf, row, width, like)
    for at in range(3):
        source_constants(jfh, at, 8, jnp.zeros((8, slots), jnp.float32))
    for copy in loads:
        copy.wait()
    slot = lax.broadcasted_iota(jnp.int32, (1, slots), 1)
    for row in range(rows):
        for cell in range(cols):
            code = jnp.where(slot < counts[row, cell], phases[row, cell : cell + 1, :] + 1, 0)
            base[6, row, cell + 1 : cell + 2, :] = code.astype(jnp.float32)
    pl.semaphore_wait(barrier, others)

    def halo(field, pack, row_got, col_got, cor_got, send, recv, par):
        copies = []
        for d, (dx, dy) in enumerate(DIRS):
            row = rows - 1 if dx > 0 else 0
            side_x, side_y = (0 if dx > 0 else 1), (0 if dy > 0 else 1)
            if dy == 0:
                src, dst = field.at[:, row], row_got.at[par, side_x]
            elif dx == 0:
                src = pack.at[1 - side_y, :, pl.ds(0, rows)]
                dst = col_got.at[par, side_y, :, pl.ds(0, rows)]
            else:
                src = pack.at[1 - side_y, :, pl.ds(row, 1)]
                dst = cor_got.at[par, :, pl.ds(2 * side_x + side_y, 1)]
            copies.append(remote(src, dst, send.at[par, d], recv.at[par, d], at_x(dx), at_y(dy)))
        return copies

    def pack_columns(field, pack, count):
        for k in range(count):
            for side, cell in enumerate((1, cols)):
                for r in range(rows):
                    pack[side, k, r : r + 1, :] = field[k, r, cell : cell + 1, :]

    def cell_rows(inner, outer, srow, col, pick):
        if 1 <= col <= cols:
            return inner[srow, pick(col, width), :]
        side = 0 if col == 0 else 1
        if srow in (0, rows + 1):
            return outer[2, pick(2 * (0 if srow == 0 else 1) + side, 8), :]
        return outer[side, pick(srow - 1, 8), :]

    def build_lhs(srow, q):
        def pick(at, step):
            return pl.ds(at, 24, stride=step)

        both = jnp.concatenate(
            [
                cell_rows(jf, jfh, srow, q, pick),
                cell_rows(jf, jfh, srow, width - 1 - q, pick),
            ],
            axis=0,
        )
        lhs[srow, q] = both.T.astype(jnp.bfloat16)

    def target_block(row, cell, ax, ay):
        at = pl.ds(cell, 8, stride=width)
        return jnp.concatenate(
            [xf[row, ax, at, :], yf[row, ay, at, :], af[row, 3 * ax + ay, at, :]], axis=0
        )

    def density_block(row, p, ax, ay):
        first = target_block(row, p + 1, ax, ay)
        second = target_block(row, cols - p, ax, 2 - ay)
        nil = jnp.zeros_like(first)
        rhs = jnp.concatenate(
            [
                jnp.concatenate([first, nil], axis=1),
                jnp.concatenate([nil, second], axis=1),
            ],
            axis=0,
        ).astype(jnp.bfloat16)
        raw = jnp.dot(lhs[row + ax, p + ay], rhs, preferred_element_type=jnp.float32)
        w = jnp.maximum(raw, 0.0)
        square = w * w
        gram[row, p, 3 * ax + ay] = square
        return jnp.sum((square * w).reshape(slots // 8, 8, 2 * slots), axis=0)

    def density_blocks(row, p, blocks, fresh):
        total = None if fresh else dsum[row, p]
        for ax, ay in blocks:
            got = density_block(row, p, ax, ay)
            total = got if total is None else total + got
        dsum[row, p] = total

    def value_cell(srow, col, ax, ay):
        def pick(group):
            return lambda at, step: pl.ds(8 * step * group + at, 8, stride=step)

        return [
            cell_rows(vf, vfh, srow, col, pick(group)) for group in (0, 1 + ax, 4 + ay)
        ]

    def force_blocks(row, p, blocks, fresh):
        left, both = [], []
        for ax, ay in blocks:
            q = p + ay
            left.append(
                jnp.concatenate(
                    value_cell(row + ax, q, ax, ay)
                    + value_cell(row + ax, width - 1 - q, ax, 2 - ay),
                    axis=0,
                ).astype(jnp.bfloat16)
            )
            g = gram[row, p, 3 * ax + ay]
            h = g.astype(jnp.bfloat16)
            left.append(left[-1])
            both.append(h)
            both.append((g - h.astype(jnp.float32)).astype(jnp.bfloat16))
        got = jnp.dot(
            jnp.concatenate(left, axis=1),
            jnp.concatenate(both, axis=0),
            preferred_element_type=jnp.float32,
        )
        for col, piece in ((p + 1, got[:24, :slots]), (cols - p, got[24:, slots:])):
            at = pl.ds(col, 24, stride=width)
            sums[row, at, :] = piece if fresh else sums[row, at, :] + piece

    every = [(ax, ay) for ax in range(3) for ay in range(3)]

    def inner_blocks(row, p):
        return [
            (ax, ay)
            for ax, ay in every
            if 1 <= row + ax <= rows and 1 <= p + ay <= cols
        ]

    def inner_phase(blocks_of, unrolled=False):
        def middle(step, carry):
            for k in range(2):
                for p in range(half):
                    blocks_of(1 + 2 * step + k, p, inner_blocks(1, p), True)
            return carry

        pairs = 0 if unrolled else (rows - 2) // 2
        if pairs:
            lax.fori_loop(0, pairs, middle, 0)
        for row in [0] + list(range(1 + 2 * pairs, rows)):
            for p in range(half):
                blocks_of(row, p, inner_blocks(row, p), True)

    def outer_phase(blocks_of, corners):
        for row in range(rows):
            for p in range(half):
                inner = inner_blocks(row, p)
                blocks = [
                    (ax, ay)
                    for ax, ay in every
                    if (ax, ay) not in inner
                    and (row + ax in (0, rows + 1) and p + ay == 0) == corners
                ]
                if blocks:
                    blocks_of(row, p, blocks, False)

    def settle(row, p):
        got = jnp.sum(dsum[row, p], axis=0, keepdims=True)
        dens[row, p + 1 : p + 2, :] = got[:, :slots]
        dens[row, cols - p : cols - p + 1, :] = got[:, slots:]

    def ratio_row(row, best):
        code = base[6, row]
        live = code > 0.5
        heavy = code > 1.5
        own = KERNEL_NORM * dens[row] / jnp.where(heavy, REST_HEAVY, REST_LIGHT)
        ratio[row] = own
        light_sel = live & jnp.logical_not(heavy)
        heavy_sel = live & heavy
        picks = ((light_sel, own), (heavy_sel, own), (light_sel, -own), (heavy_sel, -own))
        return [
            jnp.maximum(old, jnp.where(sel, value, -SENTINEL))
            for old, (sel, value) in zip(best, picks)
        ]

    def bounds_row(row, best):
        for p in range(half):
            settle(row, p)
        return ratio_row(row, best)

    def one_iteration(it, carry):
        par = lax.rem(it, 2)

        for row in range(rows):
            live = base[6, row] > 0
            for c in range(2):
                vel = base[2 + c, row] + TIME_STEP * (base[4 + c, row] + acc[c, row])
                moved = base[c, row] + TIME_STEP * vel
                pos[c, row] = jnp.where(live, moved, FAR if c == 0 else 0.0)
        pack_columns(pos, pos_pack, 2)
        pos_copies = halo(pos, pos_pack, pos_row, pos_col, pos_cor, pos_ss, pos_rs, par)
        for copy in pos_copies:
            copy.start()

        for row in range(rows):
            source_features(pos[0, row], pos[1, row], jf, row + 1, width)
            for q in range(1, half + 2):
                build_lhs(row + 1, q)
        for row in range(rows):
            target_features(pos[0, row], pos[1, row], xf, yf, af, row, width)
        inner_phase(density_blocks, True)

        for copy in pos_copies[4:]:
            copy.wait_recv()
        for side, srow in enumerate((0, rows + 1)):
            source_features(pos_row[par, side, 0], pos_row[par, side, 1], jf, srow, width)
            source_features(pos_col[par, side, 0], pos_col[par, side, 1], jfh, side, 8)
            for q in range(1, half + 2):
                build_lhs(srow, q)
        for row in range(rows):
            build_lhs(row + 1, 0)
        outer_phase(density_blocks, False)

        best = [jnp.full((width, slots), -SENTINEL, jnp.float32)] * 4
        late = [row for row in range(rows) if row in (0, rows - 1)]
        early = [row for row in range(rows) if row not in late]
        for row in early:
            best = bounds_row(row, best)
        for row in late:
            for p in range(1, half):
                settle(row, p)
        for copy in pos_copies[:4]:
            copy.wait_recv()
        source_features(pos_cor[par, 0], pos_cor[par, 1], jfh, 2, 8)
        for srow in (0, rows + 1):
            build_lhs(srow, 0)
        outer_phase(density_blocks, True)
        for row in late:
            settle(row, 0)
            best = ratio_row(row, best)
        lane = lax.broadcasted_iota(jnp.int32, (1, slots), 1)
        mine = jnp.full((1, slots), -SENTINEL, jnp.float32)
        for k in range(4):
            peak = jnp.max(jnp.max(best[k], axis=0, keepdims=True), axis=1, keepdims=True)
            mine = jnp.where(lane == k, peak, mine)
        red_snd[par] = mine
        for k, (dx, dy) in enumerate(peers):
            remote(
                red_snd.at[par],
                red_rcv.at[par, pl.ds(k, 1)],
                red_ss.at[par],
                red_rs.at[par],
                at_x(dx),
                at_y(dy),
            ).start()

        for row in range(rows):
            code = base[6, row]
            live = code > 0.5
            heavy = code > 1.5
            own = ratio[row]
            density = KERNEL_NORM * dens[row]
            safe = jnp.where(live, density, 1.0)
            scale = 1.0 / (safe * safe)
            stiff = jnp.where(heavy, STIFF_HEAVY, STIFF_LIGHT)
            beta = jnp.where(live, stiff * (own - 1.0) * scale, 0.0)
            parts[0, row] = jnp.where(live, press[row] * scale, 0.0)
            parts[1, row] = jnp.where(heavy, 0.0, beta)
            parts[2, row] = jnp.where(heavy, beta, 0.0)
        pack_columns(parts, ab_pack, 3)
        ab_copies = halo(parts, ab_pack, ab_row, ab_col, ab_cor, ab_ss, ab_rs, par)
        for copy in ab_copies:
            copy.start()

        for row in range(rows):
            value_rows(
                pos[0, row], pos[1, row], [parts[k, row] for k in range(3)], vf, row + 1, width
            )
        inner_phase(force_blocks, True)

        for copy in ab_copies[4:]:
            copy.wait_recv()
        for side, srow in enumerate((0, rows + 1)):
            value_rows(
                pos_row[par, side, 0], pos_row[par, side, 1],
                [ab_row[par, side, k] for k in range(3)], vf, srow, width,
            )
            value_rows(
                pos_col[par, side, 0], pos_col[par, side, 1],
                [ab_col[par, side, k] for k in range(3)], vfh, side, 8,
            )
        outer_phase(force_blocks, False)
        for copy in ab_copies[:4]:
            copy.wait_recv()
        value_rows(
            pos_cor[par, 0], pos_cor[par, 1], [ab_cor[par, k] for k in range(3)], vfh, 2, 8
        )
        outer_phase(force_blocks, True)

        for copy in pos_copies + ab_copies:
            copy.wait_send()
        everyone = red_rcv.at[par, pl.ds(0, others)]
        pltpu.make_async_copy(everyone, everyone, red_ss.at[par]).wait()
        pltpu.make_async_copy(everyone, everyone, red_rs.at[par]).wait()
        top = jnp.maximum(
            red_snd[par], jnp.max(red_rcv[par, 0:others, :], axis=0, keepdims=True)
        )
        bound = [
            jnp.max(jnp.where(lane == k, top, -SENTINEL), axis=1, keepdims=True)
            for k in range(4)
        ]
        bounds_out[it] = jnp.where(lane < 2, top, -top)
        relax_light = 1.0 / (1.0 + bound[0] + bound[2])
        relax_heavy = 1.0 / (1.0 + bound[1] + bound[3])

        for row in range(rows):
            def total(k):
                return sums[row, k * width : (k + 1) * width, :]

            def linear(k, mid):
                return (
                    (total(k) + total(k + mid))
                    + relax_light * (total(k + 1) + total(k + 1 + mid))
                    + relax_heavy * (total(k + 2) + total(k + 2 + mid))
                )

            code = base[6, row]
            live = code > 0.5
            heavy = code > 1.5
            relaxed = jnp.where(heavy, STIFF_HEAVY * relax_heavy, STIFF_LIGHT * relax_light)
            press[row] = jnp.where(live, press[row] + relaxed * (ratio[row] - 1.0), 0.0)
            term = parts[0, row] + relax_light * parts[1, row] + relax_heavy * parts[2, row]
            scale = jnp.where(
                heavy, 6.0 * KERNEL_NORM / MASS_HEAVY, 6.0 * KERNEL_NORM / MASS_LIGHT
            )
            plain, by_term = total(0), linear(1, 3)
            for c in range(2):
                own = pos[c, row] - 0.5
                first = 8 + 8 * c
                placed = total(first) + total(first + 4)
                force = term * (own * plain - placed) + own * by_term - linear(first + 1, 4)
                acc[c, row] = jnp.where(live, scale * force, 0.0)
        return carry

    lax.fori_loop(0, ITERS, one_iteration, 0)

    for row in range(rows):
        live = base[6, row] > 0.5
        press_out[row] = press[row]
        for c in range(2):
            vel = base[2 + c, row] + TIME_STEP * (base[4 + c, row] + acc[c, row])
            vel = jnp.where(live, vel, 0.0)
            vel_out[c, row] = vel
            pos_out[c, row] = jnp.where(live, base[c, row] + TIME_STEP * vel, 0.0)


def deliver_kernel(
    pos_in, vel_in, press_in, bounds_in, pos_out, vel_out, press_out, bounds_out, sem
):
    cols = press_out.shape[1]
    stores = [
        (press_in.at[:, pl.ds(1, cols)], press_out),
        (bounds_in, bounds_out),
    ]
    for source, target in ((pos_in, pos_out), (vel_in, vel_out)):
        for c in range(2):
            stores.append((source.at[c, :, pl.ds(1, cols)], target.at[:, :, c]))
    copies = [
        pltpu.make_async_copy(source, target, sem.at[k])
        for k, (source, target) in enumerate(stores)
    ]
    for copy in copies:
        copy.start()
    for copy in copies:
        copy.wait()


def cell_major(field):
    return jnp.transpose(field, (1, 2, 0, 3))


def slot_major(field):
    return jnp.transpose(field, (2, 0, 1, 3))


def local(position, velocity, other_accel, phase_ids, counts):
    rows, cols, slots = phase_ids.shape
    width, half = cols + 2, cols // 2
    nx, ny = lax.axis_size("gx"), lax.axis_size("gy")
    tall = -(-rows // 8) * 8
    def vm(*shape):
        return pltpu.VMEM(shape, jnp.float32)

    dma = pltpu.SemaphoreType.DMA
    held = pl.pallas_call(
        functools.partial(step_kernel, nx, ny),
        out_shape=(
            pltpu.VMEM((2, rows, width, slots), jnp.float32),
            pltpu.VMEM((2, rows, width, slots), jnp.float32),
            pltpu.VMEM((rows, width, slots), jnp.float32),
            pltpu.VMEM((ITERS, 1, slots), jnp.float32),
        ),
        in_specs=[pl.BlockSpec(memory_space=pltpu.HBM)] * 5,
        out_specs=(pl.BlockSpec(memory_space=pltpu.VMEM),) * 4,
        scratch_shapes=[
            pltpu.VMEM((rows, cols, slots), jnp.int32),
            pltpu.SMEM((rows, cols), jnp.int32),
            dma((8,)),
            vm(7, rows, width, slots),
            vm(2, rows, width, slots),
            vm(2, rows, width, slots),
            vm(rows, width, slots),
            vm(3, rows, width, slots),
            vm(rows, width, slots),
            vm(rows, width, slots),
            vm(rows, half, 8, 2 * slots),
            vm(rows + 2, 24 * width, slots),
            vm(3, 24 * tall, slots),
            pltpu.VMEM((rows + 2, half + 2, slots, 48), jnp.bfloat16),
            vm(rows, 3, 8 * width, slots),
            vm(rows, 3, 8 * width, slots),
            vm(rows, 9, 8 * width, slots),
            vm(rows + 2, 56 * width, slots),
            vm(3, 56 * tall, slots),
            vm(rows, 24 * width, slots),
            vm(rows, half, 9, slots, 2 * slots),
            vm(2, 2, tall, slots),
            vm(2, 2, 2, width, slots),
            vm(2, 2, 2, tall, slots),
            vm(2, 2, tall, slots),
            vm(2, 3, tall, slots),
            vm(2, 2, 3, width, slots),
            vm(2, 2, 3, tall, slots),
            vm(2, 3, tall, slots),
            vm(2, 1, slots),
            vm(2, nx * ny, slots),
            dma((2, 8)), dma((2, 8)), dma((2, 8)), dma((2, 8)), dma((2,)), dma((2,)),
        ],
        compiler_params=pltpu.CompilerParams(collective_id=0, has_side_effects=True, vmem_limit_bytes=40 * 2**20),
    )(*[pltpu.with_memory_space_constraint(v, pltpu.HBM) for v in (cell_major(position), cell_major(velocity), cell_major(other_accel), phase_ids, counts)])
    new_pos, new_vel, pressure, bounds = pl.pallas_call(
        deliver_kernel,
        out_shape=(
            jax.ShapeDtypeStruct((rows, cols, 2, slots), jnp.float32),
            jax.ShapeDtypeStruct((rows, cols, 2, slots), jnp.float32),
            jax.ShapeDtypeStruct((rows, cols, slots), jnp.float32),
            jax.ShapeDtypeStruct((ITERS, 1, slots), jnp.float32),
        ),
        in_specs=[pl.BlockSpec(memory_space=pl.ANY)] * 4,
        out_specs=(pl.BlockSpec(memory_space=pl.ANY),) * 4,
        scratch_shapes=[dma((6,))],
        compiler_params=pltpu.CompilerParams(vmem_limit_bytes=2**20),
    )(*held)
    return slot_major(new_pos), slot_major(new_vel), pressure, bounds[:, 0, :4]


def solution(mesh):
    placed = (
        P(None, "gx", "gy", None),
        P(None, "gx", "gy", None),
        P(None, "gx", "gy", None),
        P("gx", "gy", None),
        P("gx", "gy"),
    )
    return jax.shard_map(
        local,
        mesh=mesh,
        in_specs=placed,
        out_specs=(P(None, "gx", "gy", None), P(None, "gx", "gy", None), P("gx", "gy", None), P()),
        check_vma=False,
    )
```
